128 devices in a mesh: row: 16 (over x, y), col: 8 (over z, core).
Axes of the slice: x: 4, y: 4, z: 4, core: 2. Of those that a mesh axis runs over, the one named last changes fastest.
Arguments:
- right_sides: float32 [8, 16384, 128], P(None, ('row', 'col')), may hold values from -6 to 6
- factor_head: bfloat16 [8, 16384, 4, 1024], P(None, 'row', None, 'col'), may hold values from -0.1875 to 0.1875
- class_head: int32 [8, 16, 4], P(None, 'row'), may hold values from 0 to 2
- scale_head: float32 [8, 16, 4], P(None, 'row'), may hold values from 0.25 to 2
- inverse_head: float32 [4, 1024, 1024], P(None, 'col'), as said below
- factor_tail: bfloat16 [4, 1024, 8, 16384], P(None, 'col', None, 'row'), may hold values from -0.1875 to 0.1875
- class_tail: int32 [4, 8, 16], P(None, None, 'row'), may hold values from 0 to 2
- scale_tail: float32 [4, 8, 16], P(None, None, 'row'), may hold values from 0.25 to 2
- inverse_tail: float32 [4, 1024, 1024], P(None, None, 'col'), as said below
Outputs:
- solved_head: float32 [4, 1024, 128], P(None, 'col')
- solved_tail: float32 [4, 1024, 128], P(None, 'col')
- remainder: float32 [8, 16384, 128], P(None, ('row', 'col'))
The draws below stay inside these ranges and needn't reach their ends.
Inputs may be any that keep to these rules, and one draw needn't show every extreme that they name: `class_head`: 0, 1, 2 name the float32, bfloat16 and scaled bfloat16 classes. `class_tail`: 0, 1, 2 name the float32, bfloat16 and scaled bfloat16 classes. `inverse_head`: every tile is lower triangular with a diagonal of 1 to 2. `inverse_tail`: every tile is lower triangular with a diagonal of 1 to 2.
All inputs are finite; a program needn't handle non-finite values.
Results may differ from the reference program's by a relative error of at most 0.008.
Values sent between devices are 32-bit elements; how exact they have to be, the bound alone decides.
No kernel may reach another device: no remote copies, remote signals or barrier semaphores. Data moves between devices by JAX's collectives and lax.ppermute only.
A program may use at most 128 MiB of HBM per device.

```python
import math
import jax
import jax.numpy as jnp
from jax import lax

TILE = 1024
SLOTS = 8
RHS = 128
WIN = 4
N_ROW = 16


def lower_inverse(key):
    first_key, second_key = jax.random.split(key)
    spread = jax.random.normal(first_key, (WIN, TILE, TILE), jnp.float32) * (0.7 / math.sqrt(TILE))
    diagonal = jnp.exp(jax.random.uniform(second_key, (WIN, TILE), jnp.float32, 0.0, math.log(2.0)))
    return jnp.tril(spread, -1) + jnp.eye(TILE, dtype=jnp.float32)[None, :, :] * diagonal[:, None, :]


def draw_inverse_head(key, part):
    return lower_inverse(jax.random.fold_in(key, 11))


def draw_inverse_tail(key, part):
    return lower_inverse(jax.random.fold_in(key, 23))


def with_ends(result, rng, low, top_value):
    spot = [jax.random.randint(jax.random.fold_in(rng, axis), (), 0, length) for axis, length in enumerate(result.shape)]
    widest = result.shape.index(max(result.shape))
    neighbour = spot[:widest] + [(spot[widest] + 1) % result.shape[widest]] + spot[widest + 1:]
    return result.at[tuple(spot)].set(low).at[tuple(neighbour)].set(top_value)


def block_scale(stream_key, shape, cuts, least, high):
    def one(axis_at, parts):
        steps = jax.random.uniform(jax.random.fold_in(jax.random.fold_in(stream_key, 6), axis_at), (parts,), jnp.float32, least / len(cuts), high / len(cuts))
        return jnp.repeat(jnp.exp(steps), shape[axis_at] // parts).reshape((-1,) + (1,) * (len(shape) - axis_at - 1))

    gain = one(*cuts[0])
    for cut in cuts[1:]:
        gain = gain * one(*cut)
    return gain


def bell_draw(key, shape, width, limit, shards=(), kind=jnp.bfloat16):
    values = jax.random.normal(key, shape, jnp.float32) * width
    if len(shards) > 0:
        values = block_scale(key, shape, shards, -0.22, 0.18) * values
    return jnp.clip(values, min=-limit, max=limit).astype(kind)


def setup_inputs(seed: int = 0) -> dict:
    seeds = jax.random.split(jax.random.key(seed), 10)
    right_sides = bell_draw(seeds[0], (SLOTS, N_ROW * TILE, RHS), 1.0, 6.0, ((1, 128),), jnp.float32)
    factor_head = bell_draw(seeds[1], (SLOTS, N_ROW * TILE, WIN, TILE), TILE ** -0.5, 0.1875, ((1, 16), (3, 8)))
    class_head = with_ends(jax.random.randint(seeds[2], (SLOTS, N_ROW, WIN), 0, 3), jax.random.fold_in(seeds[2], 1), 0, 2).astype(jnp.int32)
    scale_head = jnp.clip(jnp.exp(math.log(2.0) - 2.0794415 * jax.random.uniform(seeds[3], (SLOTS, N_ROW, WIN), jnp.float32) ** block_scale(seeds[3], (SLOTS, N_ROW, WIN), ((1, 16),), -0.2, 0.2)), 0.25, 2.0)
    inverse_head = draw_inverse_head(jax.random.fold_in(seeds[9], 71), 0)
    factor_tail = bell_draw(seeds[5], (WIN, TILE, SLOTS, N_ROW * TILE), TILE ** -0.5, 0.1875, ((1, 8), (3, 16)))
    class_tail = with_ends(jax.random.randint(seeds[6], (WIN, SLOTS, N_ROW), 0, 3), jax.random.fold_in(seeds[6], 1), 0, 2).astype(jnp.int32)
    scale_tail = jnp.clip(jnp.exp(math.log(2.0) - 2.0794415 * jax.random.uniform(seeds[7], (WIN, SLOTS, N_ROW), jnp.float32) ** block_scale(seeds[7], (WIN, SLOTS, N_ROW), ((2, 16),), -0.2, 0.2)), 0.25, 2.0)
    inverse_tail = draw_inverse_tail(jax.random.fold_in(seeds[9], 71), 0)
    return dict(right_sides=right_sides, factor_head=factor_head, class_head=class_head, scale_head=scale_head, inverse_head=inverse_head, factor_tail=factor_tail, class_tail=class_tail, scale_tail=scale_tail, inverse_tail=inverse_tail)


def tile_terms(stored, classes, scales, piece, form):
    exact_piece = piece
    short_piece = piece.astype(jnp.bfloat16).astype(jnp.float32)
    wide = stored.astype(jnp.float32)
    exact_term = jnp.einsum(form, wide, exact_piece, precision=lax.Precision.HIGHEST)
    short_term = jnp.einsum(form, wide, short_piece, precision=lax.Precision.HIGHEST)
    classes = classes[:, None, None]
    scales = scales[:, None, None]
    return jnp.where(classes == 0, exact_term, jnp.where(classes == 1, short_term, scales * short_term))


def reference(right_sides, factor_head, class_head, scale_head, inverse_head, factor_tail, class_tail, scale_tail, inverse_tail):
    ntiles = SLOTS * N_ROW
    state = right_sides.reshape(SLOTS, N_ROW, TILE, RHS)
    tile_ids = jnp.arange(SLOTS, dtype=jnp.int32)[:, None] * N_ROW + jnp.arange(N_ROW, dtype=jnp.int32)[None, :]
    head_tiles = factor_head.reshape(SLOTS, N_ROW, TILE, WIN, TILE)
    heads = []
    for step in range(WIN):
        slot_k, row_k = divmod(step, N_ROW)
        solved = jnp.dot(inverse_head[step], state[slot_k, row_k], precision=lax.Precision.HIGHEST, preferred_element_type=jnp.float32)
        heads.append(solved)

        def one_slot(args):
            stored, classes, scales = args
            return tile_terms(stored, classes, scales, solved, "rab,bn->ran")

        terms = lax.map(one_slot, (head_tiles[:, :, :, step, :], class_head[:, :, step], scale_head[:, :, step]))
        active = (tile_ids > step)[:, :, None, None]
        state = state - jnp.where(active, terms, jnp.float32(0.0))
    tail_tiles = factor_tail.reshape(WIN, TILE, SLOTS, N_ROW, TILE)
    tails = [None] * WIN
    for step in range(WIN):
        target = ntiles - 1 - step
        window = WIN - 1 - step
        slot_j, row_j = divmod(target, N_ROW)
        solved = jnp.dot(inverse_tail[window].T, state[slot_j, row_j], precision=lax.Precision.HIGHEST, preferred_element_type=jnp.float32)
        tails[window] = solved
        stored_all = jnp.moveaxis(tail_tiles[window], 1, 0)

        def one_slot_back(args):
            stored, classes, scales = args
            return tile_terms(stored, classes, scales, solved, "arb,an->rbn")

        terms = lax.map(one_slot_back, (stored_all, class_tail[window], scale_tail[window]))
        active = (tile_ids < target)[:, :, None, None]
        state = state - jnp.where(active, terms, jnp.float32(0.0))
    return jnp.stack(heads), jnp.stack(tails), state.reshape(SLOTS, N_ROW * TILE, RHS)
```

```python
import functools

import jax
import jax.numpy as jnp
from jax import lax
from jax.experimental import pallas as pl
from jax.experimental.pallas import tpu as pltpu
from jax.sharding import Mesh
from jax.sharding import PartitionSpec as P

AXES = ("x", "y", "z", "c")
ROW = ("x", "y")
COL = ("z", "c")
ROW_COL = ("x", "y", "z", "c")
NX, NY, NZ, NC = 4, 4, 4, 2
STOPS = ((0, 0), (0, 1), (0, 2), (0, 3), (3, 3), (3, 2), (3, 1), (3, 0), (0, 0))
TILE = 1024
PIECE = TILE // NZ
HALF = 64
F32 = jnp.float32
BF16 = jnp.bfloat16


VMEM_LIMIT = 12 * 1024 * 1024


def device_index(x, y, z, c):
    return ((x * NY + y) * NZ + z) * NC + c


def along_z(value, shift):
    return lax.ppermute(value, "z", [(i, (i + shift) % NZ) for i in range(NZ)])


def hop(value, order, shift):
    pairs = [
        (device_index(*STOPS[i], z, c), device_index(*STOPS[i + 1], (z + shift) % NZ, c))
        for i in range(order % 2, len(STOPS) - 1, 2)
        for z in range(NZ)
        for c in range(NC)
    ]
    return lax.ppermute(value, AXES, pairs)


def core_swap(value):
    return lax.ppermute(value, "c", [(0, 1), (1, 0)])


def ring(value, axis, shift):
    return lax.ppermute(value, axis, [(i, (i + shift) % 4) for i in range(4)])


def spread(value, source):
    here = (lax.axis_index("x") == source[0]) & (lax.axis_index("y") == source[1])
    total = jnp.where(here, value, F32(0.0))
    for axis in ("y", "x"):
        parts = [ring(total, axis, shift) for shift in (1, 3, 2)]
        for part in parts:
            total = total + part
    return total


def split_two(value):
    high = value.astype(BF16)
    low = (value - high.astype(F32)).astype(BF16)
    return high, low


def pick_kernel(at_ref, kind_head_ref, scale_head_ref, kind_tail_ref, scale_tail_ref, factor_ref, head_ref, tail_ref,
                tiles_ref, inverse_ref, factor_rows_ref):
    @pl.when(at_ref[3] == 1)
    def _():
        inverse_ref[...] = head_ref[0].T

    @pl.when(at_ref[3] == 0)
    def _():
        inverse_ref[...] = tail_ref[0]

    for k in range(4):
        tiles_ref[k] = factor_ref[0, :, k, :].astype(F32).T
    slot = at_ref[0]
    for m in range(7):
        if m < 4:
            kind = kind_head_ref[slot, 0, m]
            scale = scale_head_ref[slot, 0, m]
        else:
            kind = kind_tail_ref[7 - m, 7, 0]
            scale = scale_tail_ref[7 - m, 7, 0]
        exact = jnp.where(kind == 0, F32(1.0), F32(0.0))
        factor = jnp.where(kind == 2, scale, F32(1.0))
        factor_rows_ref[2 * m : 2 * m + 1, :] = jnp.full((1, PIECE), exact, F32)
        factor_rows_ref[2 * m + 1 : 2 * m + 2, :] = jnp.full((1, PIECE), factor, F32)


def pick(at, kind_head, scale_head, kind_tail, scale_tail, factor_head, inverse_head, inverse_tail):
    smem = pl.BlockSpec(memory_space=pltpu.SMEM)
    return pl.pallas_call(
        pick_kernel,
        out_shape=[
            jax.ShapeDtypeStruct((4, 128, TILE), F32),
            jax.ShapeDtypeStruct((TILE, 128), F32),
            jax.ShapeDtypeStruct((16, PIECE), F32),
        ],
        grid_spec=pltpu.PrefetchScalarGridSpec(
            num_scalar_prefetch=1,
            grid=(1,),
            in_specs=[
                smem,
                smem,
                smem,
                smem,
                pl.BlockSpec((1, TILE, 4, 128), lambda i, at: (at[0], 0, 0, 0)),
                pl.BlockSpec((1, 128, TILE), lambda i, at: (at[1], 0, 0)),
                pl.BlockSpec((1, TILE, 128), lambda i, at: (at[2], 0, 0)),
            ],
            out_specs=[
                pl.BlockSpec((4, 128, TILE), lambda i, at: (0, 0, 0)),
                pl.BlockSpec((TILE, 128), lambda i, at: (0, 0)),
                pl.BlockSpec((16, PIECE), lambda i, at: (0, 0)),
            ],
        ),
        name="pick",
        compiler_params=pltpu.CompilerParams(vmem_limit_bytes=24 * 1024 * 1024),
    )(at, kind_head, scale_head, kind_tail, scale_tail, factor_head, inverse_head, inverse_tail)


def assemble_kernel(at_ref, right_ref, own0, own3, own1, own2a, own2b, came0, came3, came1, came2a, came2b,
                    inverse_ref, base_ref):
    z, c = at_ref[0], at_ref[1]
    half = TILE // 2
    for parts, core in (((own0, own1, own2a, own2b, own3), c), ((came0, came1, came2a, came2b, came3), 1 - c)):
        lanes = pl.ds(pl.multiple_of(core * 128, 128), 128)
        places = ((0, 0, TILE), (1, 0, TILE), (2, 0, half), (2, half, half), (3, 0, TILE))
        for ref, (shift, start, size) in zip(parts, places):
            high, low = split_two(ref[...])
            inverse_ref[0, shift, start : start + size, lanes] = high
            inverse_ref[1, shift, start : start + size, lanes] = low
    high, low = split_two(right_ref[...])
    both = jnp.concatenate([high, low], axis=0)
    rows = pl.ds(pl.multiple_of(z * PIECE, PIECE), PIECE)
    for shift in range(NZ):
        wide = jnp.dot(both, inverse_ref[0, shift, rows, :], preferred_element_type=F32)
        rest = jnp.dot(high, inverse_ref[1, shift, rows, :], preferred_element_type=F32)
        base_ref[shift] = wide[:HALF] + (wide[HALF:] + rest)


def assemble(at, right, own, came):
    vmem = pl.BlockSpec(memory_space=pltpu.VMEM)
    return pl.pallas_call(
        assemble_kernel,
        out_shape=[
            jax.ShapeDtypeStruct((2, NZ, TILE, PIECE), BF16),
            jax.ShapeDtypeStruct((NZ, HALF, PIECE), F32),
        ],
        in_specs=[pl.BlockSpec(memory_space=pltpu.SMEM)] + [vmem] * 11,
        out_specs=[vmem, vmem],
        name="assemble",
        cost_estimate=pl.CostEstimate(flops=500_000_000, bytes_accessed=8_000_000, transcendentals=0),
        compiler_params=pltpu.CompilerParams(vmem_limit_bytes=24 * 1024 * 1024),
    )(at, right, *own, *came)


def chain_tiles_kernel(at_ref, own_ref, came_ref, inverse_ref, out_ref, pair_ref):
    c, count = at_ref[0], at_ref[1]

    @pl.when(pl.program_id(0) < count)
    def _():
        pair_ref[pl.ds(pl.multiple_of(c * 128, 128), 128), :] = own_ref[0].astype(BF16)
        pair_ref[pl.ds(pl.multiple_of((1 - c) * 128, 128), 128), :] = came_ref[0].astype(BF16)
        pair = pair_ref[...]
        for shift in range(NZ):
            product = jnp.dot(pair, inverse_ref[0, shift], preferred_element_type=F32)
            product = product + jnp.dot(pair, inverse_ref[1, shift], preferred_element_type=F32)
            high, low = split_two(product)
            out_ref[0, 0, shift] = high
            out_ref[0, 1, shift] = low


def chain_tiles(at, own, came, inverse):
    count = own.shape[0]

    def place(m, at):
        return (jnp.minimum(m, jnp.maximum(at[1], 1) - 1), 0, 0)

    block = pl.BlockSpec((1, 128, TILE), place)
    return pl.pallas_call(
        chain_tiles_kernel,
        out_shape=jax.ShapeDtypeStruct((count, 2, NZ, PIECE, PIECE), BF16),
        grid_spec=pltpu.PrefetchScalarGridSpec(
            num_scalar_prefetch=1,
            grid=(count,),
            in_specs=[block, block, pl.BlockSpec((2, NZ, TILE, PIECE), lambda m, at: (0, 0, 0, 0))],
            out_specs=pl.BlockSpec((1, 2, NZ, PIECE, PIECE), lambda m, at: (*place(m, at), 0, 0)),
            scratch_shapes=[pltpu.VMEM((PIECE, TILE), BF16)],
        ),
        name="chain_tiles",
        cost_estimate=pl.CostEstimate(flops=2_000_000_000, bytes_accessed=8_000_000, transcendentals=0),
        compiler_params=pltpu.CompilerParams(vmem_limit_bytes=24 * 1024 * 1024),
    )(at, own, came, inverse)


def tile_operand(value, rows_ref, m):
    high, low = split_two(value)
    used = high.astype(F32) + low.astype(F32) * rows_ref[2 * m : 2 * m + 1, :]
    return split_two(used * rows_ref[2 * m + 1 : 2 * m + 2, :])


def tile_product(operand, tile_ref, m, shift):
    high, low = operand
    wide = jnp.dot(jnp.concatenate([high, low], axis=0), tile_ref[m, 0, shift], preferred_element_type=F32)
    rest = jnp.dot(high, tile_ref[m, 1, shift], preferred_element_type=F32)
    return wide[:HALF] + (wide[HALF:] + rest)


def early_kernel(count, rows_ref, base_ref, before_ref, head_ref, *rest):
    *tails, out_ref = rest
    operands = [tile_operand(before_ref[m], rows_ref, m) for m in range(count)]
    for shift in range(NZ):
        total = base_ref[shift]
        for m in range(count):
            if m < 4:
                total = total - tile_product(operands[m], head_ref, m, shift)
            else:
                total = total - tile_product(operands[m], tails[0], m - 4, shift)
        out_ref[shift] = total


def early(count, rows, base, before, head, tail):
    args = [rows, base, before, head] + ([tail] if count > 4 else [])
    vmem = pl.BlockSpec(memory_space=pltpu.VMEM)
    return pl.pallas_call(
        functools.partial(early_kernel, count),
        out_shape=jax.ShapeDtypeStruct((NZ, HALF, PIECE), F32),
        in_specs=[vmem] * len(args),
        out_specs=vmem,
        name=f"early_{count}",
        cost_estimate=pl.CostEstimate(flops=1_000_000_000, bytes_accessed=1_000_000, transcendentals=0),
        compiler_params=pltpu.CompilerParams(vmem_limit_bytes=VMEM_LIMIT),
    )(*args)


def step_kernel(order, rows_ref, early_ref, tile_ref, h0, h1, h2, h3, *refs):
    if order > 1:
        before_ref, all_ref, *outs = refs
    else:
        all_ref, *outs = refs
    newest = (h0[...] + h1[...]) + (h2[...] + h3[...])
    for i in range(order - 1):
        all_ref[i] = before_ref[i]
    all_ref[order - 1] = newest
    operand = tile_operand(newest, rows_ref, order - 1)
    for shift, out in enumerate(outs):
        out[...] = early_ref[shift] - tile_product(operand, tile_ref, (order - 1) % 4, shift)


def step_call(order, rows, sooner, head, tail, pieces, before):
    args = [rows, sooner, head if order <= 4 else tail, *pieces] + ([before] if order > 1 else [])
    vmem = pl.BlockSpec(memory_space=pltpu.VMEM)
    return pl.pallas_call(
        functools.partial(step_kernel, order),
        out_shape=[jax.ShapeDtypeStruct((order, HALF, PIECE), F32)]
        + [jax.ShapeDtypeStruct((HALF, PIECE), F32)] * NZ,
        in_specs=[vmem] * len(args),
        out_specs=[vmem] * (NZ + 1),
        name=f"step_{order}",
        cost_estimate=pl.CostEstimate(flops=1_000_000_000, bytes_accessed=1_000_000, transcendentals=0),
        compiler_params=pltpu.CompilerParams(vmem_limit_bytes=VMEM_LIMIT),
    )(*args)


def on_device(
    right_sides,
    factor_head,
    class_head,
    scale_head,
    inverse_head,
    factor_tail,
    class_tail,
    scale_tail,
    inverse_tail,
):
    x, y, z, c = (lax.axis_index(a) for a in AXES)
    slots = right_sides.shape[0]
    first = x == 0

    use_head = first.astype(jnp.int32)
    at = jnp.stack([jnp.where(first, 0, slots - 1), y, y, use_head]).astype(jnp.int32)
    own_head, own_inverse, rows = pick(
        at, class_head, scale_head, class_tail, scale_tail, factor_head, inverse_head, inverse_tail
    )
    below, above = along_z(own_inverse, 1), along_z(own_inverse, 3)
    half = TILE // 2
    own = [own_inverse, below, above, along_z(below[:half], 1), along_z(above[half:], 3)]
    came = [core_swap(part) for part in own]
    came_head = core_swap(own_head)
    own_tail = factor_tail[::-1][:3, :, slots - 1, :].astype(F32)
    came_tail = core_swap(own_tail)

    right = jnp.where(first, right_sides[0], right_sides[slots - 1]).T
    low, high = right[:HALF], right[HALF:]
    mine = jnp.where(c == 0, low, high)
    theirs = core_swap(jnp.where(c == 0, high, low))
    right_piece = jnp.where(
        c == 0, jnp.concatenate([mine, theirs], axis=1), jnp.concatenate([theirs, mine], axis=1)
    )

    place = jnp.stack([z, c]).astype(jnp.int32)
    inverse, base = assemble(place, right_piece, own, came)
    rank = jnp.where(first, y, jnp.where(x == 3, 7 - y, 0))
    head = chain_tiles(jnp.stack([c, jnp.minimum(rank, 4)]).astype(jnp.int32), own_head, came_head, inverse)
    tail = chain_tiles(jnp.stack([c, jnp.maximum(rank - 4, 0)]).astype(jnp.int32), own_tail, came_tail, inverse)

    outs = [base[shift] for shift in range(NZ)]
    known = before = heads = None
    sooner = base
    for order in range(1, len(STOPS)):
        pieces = [hop(outs[shift], order - 1, shift) for shift in range(NZ)]
        if order > 1:
            before = hop(known, order - 1, 0)
            if order < len(STOPS) - 1:
                sooner = early(order - 1, rows, base, before, head, tail)
        if order < len(STOPS) - 1:
            known, *outs = step_call(order, rows, sooner, head, tail, pieces, before)
        if order == 4:
            heads = spread(known, STOPS[order])
    newest = (pieces[0] + pieces[1]) + (pieces[2] + pieces[3])
    tails = spread(jnp.concatenate([before[4:], newest[None]], axis=0), STOPS[-1])

    def whole(parts):
        mine = jnp.where(c == 0, parts[..., :128], parts[..., 128:])
        came = core_swap(jnp.where(c == 0, parts[..., 128:], parts[..., :128]))
        return jnp.where(
            c == 0, jnp.concatenate([mine, came], axis=1), jnp.concatenate([came, mine], axis=1)
        )

    heads = whole(heads)
    tails = whole(tails)[::-1]
    row = x * NY + y
    tile_ids = jnp.arange(slots, dtype=jnp.int32) * (NX * NY) + row

    def operand(solved, kinds, scales, active):
        kinds, scales, active = (a[:, :, None, None] for a in (kinds, scales, active))
        rounded = lax.reduce_precision(solved, 8, 7)[None]
        values = jnp.where(kinds == 0, solved[None], rounded)
        factor = jnp.where(active, jnp.where(kinds == 2, scales, F32(1.0)), F32(0.0))
        return (values * factor).astype(BF16)

    steps = jnp.arange(4, dtype=jnp.int32)
    head_operand = operand(heads, class_head[:, 0], scale_head[:, 0], tile_ids[:, None] > steps[None, :])
    tail_operand = operand(
        tails,
        class_tail[:, :, 0].T,
        scale_tail[:, :, 0].T,
        tile_ids[:, None] < (slots * NX * NY - 4 + steps)[None, :],
    )
    updates = jnp.einsum("lakb,lknb->lan", factor_head, head_operand, preferred_element_type=F32)
    updates = updates + jnp.einsum("walb,lwna->lbn", factor_tail, tail_operand, preferred_element_type=F32)
    updates = updates.reshape(slots, NZ, NC, 128, 128)
    updates = jnp.where(c == 0, updates[:, :, 0], updates[:, :, 1]) + core_swap(
        jnp.where(c == 0, updates[:, :, 1], updates[:, :, 0])
    )
    blocks = [
        lax.dynamic_index_in_dim(updates, lax.rem(z + shift, NZ), 1, keepdims=False) for shift in range(NZ)
    ]
    parts = [along_z(blocks[shift], shift) for shift in (1, 3, 2)]
    summed = (blocks[0] + parts[0]) + (parts[1] + parts[2])
    return jnp.swapaxes(heads, 1, 2), jnp.swapaxes(tails, 1, 2), right_sides - summed


def solution(mesh):
    finer = Mesh(mesh.devices.reshape(NX, NY, NZ, NC), AXES)
    return jax.shard_map(
        on_device,
        mesh=finer,
        in_specs=(
            P(None, ROW_COL, None),
            P(None, ROW, None, COL),
            P(None, ROW, None),
            P(None, ROW, None),
            P(None, COL, None),
            P(None, COL, None, ROW),
            P(None, None, ROW),
            P(None, None, ROW),
            P(None, None, COL),
        ),
        out_specs=(P(None, COL, None), P(None, COL, None), P(None, ROW_COL, None)),
        check_vma=False,
    )
```
